32 devices in a mesh: ta: 16 (over z, y, x), sa: 2 (over core).
Axes of the slice: x: 2, y: 2, z: 4, core: 2. Of those that a mesh axis runs over, the one named last changes fastest.
Arguments:
- rhs: float32 [1, 2, 40, 16, 2, 128], P(None, None, None, 'ta', 'sa'), may hold values from -6 to 6
- links: bfloat16 [4, 2, 40, 40, 16, 2, 128], P(None, None, None, None, 'ta', 'sa'), may hold values from -0.625 to 0.625
- clover: bfloat16 [2, 40, 40, 16, 2, 128], P(None, None, None, 'ta', 'sa'), may hold values from -1 to 7
- mr_steps: int32 [16, 2, 2], P('ta', 'sa'), may hold values from 2 to 3
Outputs:
- solution: float32 [1, 2, 40, 16, 2, 128], P(None, None, None, 'ta', 'sa')
- residual: float32 [1, 2, 40, 16, 2, 128], P(None, None, None, 'ta', 'sa')
The draws below stay inside these ranges and needn't reach their ends.
All inputs are finite; a program needn't handle non-finite values.
Results may differ from the reference program's by a relative error of at most 0.0003.
Values sent between devices are 32-bit elements; how exact they have to be, the bound alone decides.
A program may use at most 128 MiB of HBM per device.

```python
import jax
import jax.numpy as jnp
from jax import lax

NVEC = 20
DOF = 40
NRHS = 1
TD = 2
LZ = 4
LY = 4
LX = 4
MR_MAX = 3
SWEEPS = 2
NTD = 16
NZD = 2
DS = 128


def draw_clover(key, part):
    folded = jax.random.fold_in(key, 7)
    first, second = jax.random.split(folded)
    shape = (2, DOF, DOF, NTD, NZD, DS)
    spread = jax.random.normal(first, shape, jnp.float32) / jnp.sqrt(jnp.float32(DOF))
    diagonal = jax.random.uniform(second, (NTD, NZD, DS), jnp.float32, 3.5, 5.0)
    spread = jnp.clip(spread, -1.0, 1.0)
    identity = jnp.eye(DOF, dtype=jnp.float32)[:, :, None, None, None]
    real_part = spread[0] + identity * diagonal[None, None]
    return jnp.stack([real_part, spread[1]], 0).astype(jnp.bfloat16)


def with_ends(array, rng, low, largest):
    spot = [jax.random.randint(jax.random.fold_in(rng, axis), (), 0, length) for axis, length in enumerate(array.shape)]
    longest = array.shape.index(max(array.shape))
    neighbour = spot[:longest] + [(spot[longest] + 1) % array.shape[longest]] + spot[longest + 1:]
    return array.at[tuple(spot)].set(low).at[tuple(neighbour)].set(largest)


def levels(own_key, shape, cuts, smallest, top_value):
    factor_of = 1.0
    for axis_at, shards_of in cuts:
        draws = jax.random.uniform(jax.random.fold_in(jax.random.fold_in(own_key, 6), axis_at), (shards_of,), jnp.float32, smallest / len(cuts), top_value / len(cuts))
        factor_of = factor_of * jnp.repeat(jnp.exp(draws), shape[axis_at] // shards_of).reshape((-1,) + (1,) * (len(shape) - 1 - axis_at))
    return factor_of


def bell_draw(own_key, shape, deviation, most, cuts=(), kind=jnp.bfloat16):
    values = deviation * jax.random.normal(own_key, shape, jnp.float32)
    if cuts:
        values = values * levels(own_key, shape, cuts, -0.22, 0.18)
    return jnp.clip(values, -most, most).astype(kind)


def setup_inputs(seed: int = 0) -> dict:
    key_list = jax.random.split(jax.random.key(seed), 5)
    rhs = bell_draw(key_list[0], (NRHS, 2, DOF, NTD, NZD, DS), 1.0, 6.0, ((3, 16), (4, 2)), jnp.float32)
    links = bell_draw(key_list[1], (4, 2, DOF, DOF, NTD, NZD, DS), (2 * DOF) ** -0.5, 0.625, ((4, 16), (5, 2)))
    clover = draw_clover(jax.random.fold_in(key_list[4], 71), 0)
    mr_steps = with_ends(jax.random.randint(key_list[3], (NTD, NZD, 2), 2, MR_MAX + 1), jax.random.fold_in(key_list[3], 1), 2, MR_MAX).astype(jnp.int32)
    return {"rhs": rhs, "links": links, "clover": clover, "mr_steps": mr_steps}


HIGHEST = lax.Precision.HIGHEST


def complex_apply(matrices, vectors, dagger):
    real_mat = matrices[0].astype(jnp.float32)
    imag_mat = matrices[1].astype(jnp.float32)
    real_vec = vectors[:, 0]
    imag_vec = vectors[:, 1]
    pattern = "ji...,rj...->ri..." if dagger else "ij...,rj...->ri..."

    def product(left, right):
        return jnp.einsum(pattern, left, right, precision=HIGHEST)

    if dagger:
        real_out = product(real_mat, real_vec) + product(imag_mat, imag_vec)
        imag_out = product(real_mat, imag_vec) - product(imag_mat, real_vec)
    else:
        real_out = product(real_mat, real_vec) - product(imag_mat, imag_vec)
        imag_out = product(real_mat, imag_vec) + product(imag_mat, real_vec)
    return jnp.stack([real_out, imag_out], axis=1)


def lattice_view(field):
    leading = field.shape[:3]
    shaped = field.reshape(leading + (NTD, NZD, TD, LZ, LY, LX))
    shaped = jnp.transpose(shaped, (0, 1, 2, 3, 5, 4, 6, 7, 8))
    return shaped.reshape(leading + (NTD * TD, NZD * LZ, LY, LX))


def domain_view(lattice):
    leading = lattice.shape[:3]
    shaped = lattice.reshape(leading + (NTD, TD, NZD, LZ, LY, LX))
    shaped = jnp.transpose(shaped, (0, 1, 2, 3, 5, 4, 6, 7, 8))
    return shaped.reshape(leading + (NTD, NZD, DS))


def shifted(field, direction, amount):
    return domain_view(jnp.roll(lattice_view(field), amount, axis=3 + direction))


def apply_operator(field, links, clover):
    signs = jnp.where(jnp.arange(DOF) < NVEC, 1.0, -1.0).astype(jnp.float32)[:, None, None]

    def backward_terms(index):
        vectors = lax.dynamic_index_in_dim(field, index, 3, keepdims=False)
        matrices = lax.dynamic_index_in_dim(links, index, 4, keepdims=False)
        return jnp.stack([signs * complex_apply(matrices[direction], signs * vectors, True) for direction in range(4)], 0)

    back_terms = jnp.moveaxis(lax.map(backward_terms, jnp.arange(NTD)), 0, 4)
    neighbours = jnp.stack([shifted(field, direction, -1) for direction in range(4)], 0)
    behind_total = shifted(back_terms[0], 0, 1)
    for direction in range(1, 4):
        behind_total = behind_total + shifted(back_terms[direction], direction, 1)

    def forward_terms(index):
        vectors = lax.dynamic_index_in_dim(field, index, 3, keepdims=False)
        nearby = lax.dynamic_index_in_dim(neighbours, index, 4, keepdims=False)
        matrices = lax.dynamic_index_in_dim(links, index, 4, keepdims=False)
        self_block = lax.dynamic_index_in_dim(clover, index, 3, keepdims=False)
        total = complex_apply(self_block, vectors, False)
        for direction in range(4):
            total = total - complex_apply(matrices[direction], nearby[direction], False)
        return total

    result = jnp.moveaxis(lax.map(forward_terms, jnp.arange(NTD)), 0, 3)
    return result - behind_total


def block_sums(component):
    shaped = component.reshape(component.shape[:4] + (2, DS // 2))
    return jnp.sum(shaped, axis=(1, 5))


def block_scale(factor, component):
    shaped = component.reshape(component.shape[:4] + (2, DS // 2))
    return (factor[:, None, :, :, :, None] * shaped).reshape(component.shape)


def reference(rhs, links, clover, mr_steps):
    colour = (jnp.arange(DS)[None, :] // (DS // 2) + jnp.arange(NZD)[:, None]) % 2
    solution = jnp.zeros_like(rhs)
    for sweep_index in range(SWEEPS):
        for colour_index in range(2):
            mask = (colour == colour_index).astype(jnp.float32)
            remainder = rhs - apply_operator(solution, links, clover)
            search = remainder * mask
            correction = jnp.zeros_like(search)
            for step_index in range(MR_MAX):
                image = apply_operator(search, links, clover) * mask
                real_s = search[:, 0]
                imag_s = search[:, 1]
                real_q = image[:, 0]
                imag_q = image[:, 1]
                numer_real = block_sums(real_q * real_s + imag_q * imag_s)
                numer_imag = block_sums(real_q * imag_s - imag_q * real_s)
                denom = block_sums(real_q * real_q + imag_q * imag_q) + 1e-6
                live = (step_index < mr_steps)[None]
                alpha_real = jnp.where(live, numer_real / denom, 0.0)
                alpha_imag = jnp.where(live, numer_imag / denom, 0.0)
                correction = correction + jnp.stack([block_scale(alpha_real, real_s) - block_scale(alpha_imag, imag_s), block_scale(alpha_real, imag_s) + block_scale(alpha_imag, real_s)], 1)
                search = search - jnp.stack([block_scale(alpha_real, real_q) - block_scale(alpha_imag, imag_q), block_scale(alpha_real, imag_q) + block_scale(alpha_imag, real_q)], 1)
            solution = solution + correction
    residual = rhs - apply_operator(solution, links, clover)
    return solution, residual
```

```python
import functools

import jax
import jax.numpy as jnp
from jax import lax
from jax.experimental import pallas as pl
from jax.experimental.pallas import tpu as pltpu
from jax.sharding import PartitionSpec as P

LZ = 4
LY = 4
LX = 4
MR_MAX = 3
SWEEPS = 2
PHASES = 2 * SWEEPS
PREPARE_UNROLL = 8
MESH = pl.DeviceIdType.MESH
F32 = jnp.float32
BF16 = jnp.bfloat16


def rows_of(dof):
    whole = dof // 16
    return [(16 * t, 16) for t in range(whole)] + [(16 * whole, dof - 16 * whole)]


def kernel(
    nt,
    nz,
    rhs_hbm,
    links_ref,
    clover_ref,
    steps_hbm,
    x_ref,
    r_ref,
    rhs_ref,
    steps_ref,
    lk,
    cl,
    gf,
    gb,
    gh,
    xr,
    rs,
    xs,
    v_ref,
    q_ref,
    s_ref,
    e_ref,
    bs_ref,
    acc,
    t_ref,
    gv,
    opf,
    pk,
    f_ref,
    sbuf,
    rbuf,
    csem,
    ssem,
    rsem,
):
    dof, lanes = rhs_ref.shape[1:]
    half = lanes // 2
    tiles = dof // 8
    whole = dof // 16
    packed = 2 * dof // 16
    pieces = rows_of(dof)
    ta = lax.axis_index("ta")
    sa = lax.axis_index("sa")
    t_next, t_prev = lax.rem(ta + 1, nt), lax.rem(ta + nt - 1, nt)
    z_next, z_prev = lax.rem(sa + 1, nz), lax.rem(sa + nz - 1, nz)

    copies = [
        pltpu.make_async_copy(links_ref.at[d], lk.at[d], csem.at[d]) for d in range(4)
    ] + [
        pltpu.make_async_copy(clover_ref, cl, csem.at[4]),
        pltpu.make_async_copy(rhs_hbm, rhs_ref, csem.at[5]),
        pltpu.make_async_copy(steps_hbm, steps_ref, csem.at[6]),
    ]
    for d in (5, 6, 1, 2, 3, 4, 0):
        copies[d].start()

    barrier = pltpu.get_barrier_semaphore()
    for where_to in ({"ta": t_next}, {"ta": t_prev}, {"sa": z_next}, {"sa": z_prev}):
        pl.semaphore_signal(barrier, inc=1, device_id=where_to, device_id_type=MESH)

    shape = (dof, lanes)
    lane = lax.broadcasted_iota(jnp.int32, shape, 1)
    row = lax.broadcasted_iota(jnp.int32, shape, 0)
    signs = jnp.where(row < dof // 2, 1.0, -1.0).astype(F32)
    low = lane < half
    site = lane % half
    zpos = site // (LY * LX)
    ypos = site // LX % LY
    xpos = site % LX
    z_last, z_first = zpos == LZ - 1, zpos == 0
    y_last, y_first = ypos == LY - 1, ypos == 0
    x_last, x_first = xpos == LX - 1, xpos == 0
    zero = jnp.zeros(shape, F32)
    plane = LY * LX

    def roll(v, by):
        return pltpu.roll(v, by % lanes, 1)

    def first_rows(h, rows):
        at = lax.broadcasted_iota(jnp.int32, (rows, lanes), 1)
        return jnp.where((at >= half) == ((at * 0 + h) == 1), 1.0, 0.0).astype(BF16) > 0.5

    def loop(body):
        def block(outer, carry):
            for inner in range(PREPARE_UNROLL):
                body(outer * PREPARE_UNROLL + inner)
            return carry

        lax.fori_loop(0, dof // PREPARE_UNROLL, block, 0)

    def prepare(h, stage):
        masks = {rows: first_rows(h, rows) for _, rows in pieces}

        def store(ref, i, base, top, c, at, rows, value):
            if rows == 16:
                ref[h, i, base + 16 * whole * c + at : base + 16 * whole * c + at + 16, :] = value
            else:
                ref[h, i, base + 32 * whole + 8 * c : base + 32 * whole + 8 * c + 8, :] = value

        def body(i):
            for c in range(2):
                for at, rows in pieces:
                    cut = slice(at, at + rows)
                    first = masks[rows]
                    if stage == 0:
                        z = pltpu.roll(lk[1, c, i, cut, :], half, 1)
                        g = jnp.where(first, lk[2, c, i, cut, :], z)
                        store(gf, i, 0, 0, c, at, rows, g)
                        store(gb, i, 2 * dof * c, 0, 0, at, rows, g)
                    if stage == 1:
                        x = pltpu.roll(lk[3, c, i, cut, :], half, 1)
                        xr[c, i, cut, :] = x
                        store(gf, i, 2 * dof, 0, c, at, rows, jnp.where(first, cl[c, i, cut, :], x))
                    if stage == 2:
                        g = jnp.where(first, lk[0, c, i, cut, :], xr[c, i, cut, :])
                        store(gb, i, 2 * dof * c, 0, 1, at, rows, g)
                    if stage == 3:
                        z = pltpu.roll(lk[1, c, i, cut, :], half, 1)
                        store(gh, i, 0, 0, c, at, rows, jnp.where(first, lk[0, c, i, cut, :], z))

        loop(body)

    copies[5].wait()
    for c in range(2):
        v = rhs_ref[c]
        w = roll(v, half)
        rs[0, c] = jnp.where(low, v, w)
        rs[1, c] = jnp.where(low, w, v)
        xs[0, c] = zero
        xs[1, c] = zero

    for stage, needs in enumerate(((1, 2), (3, 4), (0, 6))):
        for d in needs:
            copies[d].wait()
        prepare(sa % 2, stage)

    def fold(v):
        total = v[0:8]
        for t in range(1, tiles):
            total = total + v[8 * t : 8 * t + 8]
        return total

    def gathered(slot):
        parts = []
        for t in range(tiles):
            total = None
            for k in range(8):
                piece = f_ref[slot, pl.ds(8 * 8 * t + k, 8, stride=8), :]
                total = piece if total is None else total + piece
            parts.append(total)
        return jnp.concatenate(parts, axis=0)

    def two(v):
        high = v.astype(BF16).astype(F32)
        return high, v - high

    def put_operands(slot, group, vr, vi):
        for term, (r, i) in enumerate(zip(two(vr), two(vi))):
            n = -i
            top = 16 * whole
            out = [r[16 * t : 16 * t + 16] for t in range(whole)]
            out += [i[16 * t : 16 * t + 16] for t in range(whole)]
            out += [n[16 * t : 16 * t + 16] for t in range(whole)]
            out += [jnp.concatenate([r[top:], n[top:]], axis=0), jnp.concatenate([i[top:], r[top:]], axis=0)]
            for at, value in enumerate(out):
                opf[slot, group, term, at] = value.astype(BF16)

    def forward(slot, groups, matrix):
        def operand(group, term, at):
            return opf[slot, group, term, at].astype(F32)

        real = list(range(whole)) + list(range(2 * whole, 3 * whole)) + [3 * whole]
        imag = list(range(whole, 2 * whole)) + list(range(whole)) + [3 * whole + 1]
        for o in range(dof):
            sums = [None, None]
            for group in range(groups):
                for t in range(packed):
                    m = matrix(o, group, t).astype(F32)
                    for term in range(2):
                        for part, order in enumerate((real, imag)):
                            p = m * operand(group, term, order[t])
                            sums[part] = p if sums[part] is None else sums[part] + p
            for part in range(2):
                f_ref[part, 8 * o : 8 * o + 8, :] = sums[part][0:8] + sums[part][8:16]

    def backward(slot, matrix):
        rounds = []
        t = 0
        while t + 1 < packed:
            rounds.append([(t, 0, dof), (t + 1, 0, dof)])
            t += 2
        if t < packed:
            rounds.append([(t, 0, dof // 2), (t, dof // 2, dof)])
        done = {}
        for index, chains in enumerate(rounds):
            sums = [[None, None] for _ in chains]
            for step in range(chains[0][2] - chains[0][1]):
                if index == 0:
                    for n in range(6):
                        spread = jnp.broadcast_to(gv[n, pl.ds(step, 1), :], (16, lanes))
                        pk[slot, n, step] = spread.astype(BF16)
                for chain, (t, start, _) in enumerate(chains):
                    i = start + step
                    mr = matrix(i, 0, t).astype(F32)
                    mi = matrix(i, 1, t).astype(F32)
                    x = [pk[slot, n, i].astype(F32) for n in range(6)]
                    for part, terms in enumerate(
                        (
                            ((mr, x[0]), (mr, x[1]), (mi, x[2]), (mi, x[3])),
                            ((mr, x[2]), (mr, x[3]), (mi, x[4]), (mi, x[5])),
                        )
                    ):
                        for m, y in terms:
                            p = m * y
                            old = sums[chain][part]
                            sums[chain][part] = p if old is None else old + p
            for chain, (t, _, _) in enumerate(chains):
                if t in done:
                    done[t] = [a + b for a, b in zip(done[t], sums[chain])]
                else:
                    done[t] = sums[chain]
        out = []
        for group in range(2):
            out.append([])
            for part in range(2):
                parts = [done[whole * group + t][part] for t in range(whole)]
                parts.append(done[2 * whole][part][8 * group : 8 * group + 8])
                out[group].append(-signs * jnp.concatenate(parts, axis=0))
        return out

    def phase(ph, token):
        h = lax.rem(ph + sa, 2)
        other = 1 - h
        limit = steps_ref[h]
        first = (lane >= half) == ((lane * 0 + h) == 1)
        h_is_0 = (lane * 0 + h) == 0

        def ahead(v):
            n = -v
            ya = jnp.where(y_last, roll(n, (LY - 1) * LX), roll(n, -LX))
            za = jnp.where(z_last, 0.0, roll(n, -plane))
            xa = jnp.where(x_last, roll(n, LX - 1), roll(n, -1))
            return jnp.where(first, ya, za), jnp.where(first, v, xa)

        for c in range(2):
            v = rs[h, c]
            v_ref[c] = v
            s_ref[c] = v
            e_ref[c] = v
            q_ref[c] = zero
            for n in range(2):
                acc[n, c] = zero
                bs_ref[n, c] = zero

        def total(v):
            return jnp.sum(jnp.sum(fold(v), axis=0, keepdims=True), axis=1, keepdims=True)

        def scale(k):
            qr, qi, sr, si = q_ref[0], q_ref[1], s_ref[0], s_ref[1]
            numer_real = total(qr * sr + qi * si)
            numer_imag = total(qr * si - qi * sr)
            denom = total(qr * qr + qi * qi) + 2e-6
            live = (lane * 0 + limit) > k
            ar = jnp.where(live, jnp.broadcast_to(numer_real / denom, shape), 0.0)
            ai = jnp.where(live, jnp.broadcast_to(numer_imag / denom, shape), 0.0)
            return ar, ai

        def times(ar, ai, v):
            return ar * v[0] - ai * v[1], ar * v[1] + ai * v[0]

        def step(k, carry):
            ar, ai = scale(k - 1)
            opening = (lane * 0 + k) == 0
            ar = jnp.where(opening, -1.0, ar)
            ai = jnp.where(opening, 0.0, ai)

            vr, vi = v_ref[0], v_ref[1]
            gr, gi = two(signs * vr), two(signs * vi)
            for term in range(2):
                gv[term] = gr[term]
                gv[2 + term] = gi[term]
                gv[4 + term] = -gr[term]

            aheads = [ahead(vr), ahead(vi)]
            for group in range(2):
                put_operands(k, group, aheads[0][group], aheads[1][group])

            back0, back2 = backward(
                k, lambda i, c, t: gb[h, i, 2 * dof * c + 16 * t : 2 * dof * c + 16 * t + 16, :]
            )
            near, moved = [], []
            for c in range(2):
                b, d = back0[c], back2[c]
                yb = jnp.where(y_first, roll(b, -(LY - 1) * LX), roll(b, LX))
                zb = jnp.where(z_first, 0.0, roll(b, plane))
                xb = jnp.where(x_first, roll(d, -(LX - 1)), roll(d, 1))
                u = jnp.where(first, yb, zb) + jnp.where(first, 0.0, xb)
                near.append(u + roll(u, half))
                moved.append((jnp.where(first, roll(b, half), b), jnp.where(first, d, roll(d, half))))

            forward(
                k,
                2,
                lambda o, group, t: gf[h, o, 2 * dof * group + 16 * t : 2 * dof * group + 16 * t + 16, :],
            )

            old_s = (s_ref[0], s_ref[1])
            old_q = (q_ref[0], q_ref[1])
            es = times(ar, ai, old_s)
            qs = times(ar, ai, old_q)
            for c in range(2):
                e_ref[c] += es[c]
                s_ref[c] = old_s[c] - qs[c]
            for n in range(2):
                old_b = (bs_ref[n, 0], bs_ref[n, 1])
                now = (moved[0][n], moved[1][n])
                added = times(ar, ai, old_b)
                taken = times(ar, ai, now)
                for c in range(2):
                    acc[n, c] += added[c]
                    bs_ref[n, c] = old_b[c] - taken[c]
            w = []
            for c in range(2):
                u = gathered(c)
                w.append(u + roll(u, half) + near[c])
            ws = times(ar, ai, w)
            for c in range(2):
                q = old_q[c] - ws[c]
                q_ref[c] = q
                v_ref[c] = q
            return carry

        lax.fori_loop(0, MR_MAX, step, 0)

        def pack(v):
            return jnp.where(low, v[0], v[1])

        def sender(n, where_to, src, dst):
            return pltpu.make_async_remote_copy(
                src_ref=src,
                dst_ref=dst,
                send_sem=ssem.at[ph, n],
                recv_sem=rsem.at[ph, n],
                device_id=where_to,
                device_id_type=MESH,
            )

        target = {"ta": lax.rem(ta + nt + 2 * h - 1, nt)}

        @pl.when(ph == 0)
        def _():
            pl.semaphore_wait(barrier, 4)

        ar, ai = scale(MR_MAX - 1)
        es = times(ar, ai, (s_ref[0], s_ref[1]))
        e_new = [e_ref[c] + es[c] for c in range(2)]
        added = times(ar, ai, (bs_ref[1, 0], bs_ref[1, 1]))
        bt = [-(acc[1, c] + added[c]) for c in range(2)]
        sbuf[ph, 0] = jnp.where(h_is_0, pack(e_new), pack(bt))
        sends = [sender(0, target, sbuf.at[ph, 0], rbuf.at[ph, 0])]
        sends[0].start()
        bs = times(ar, ai, (bs_ref[0, 0], bs_ref[0, 1]))
        bz = [-(acc[0, c] + bs[c]) for c in range(2)]
        sbuf[ph, 1] = pack(e_new)
        sbuf[ph, 2] = pack(bz)
        sends.append(sender(1, {"sa": z_prev}, sbuf.at[ph, 1], rbuf.at[ph, 1]))
        sends.append(sender(2, {"sa": z_next}, sbuf.at[ph, 2], rbuf.at[ph, 2]))
        sends[1].start()
        sends[2].start()

        qs = times(ar, ai, (q_ref[0], q_ref[1]))
        for c in range(2):
            xs[h, c] += e_new[c]
            rs[h, c] = s_ref[c] - qs[c]

        @pl.when(h == 0)
        def _():
            for c in range(2):
                rs[1, c] += bt[c]

        @pl.when(h == 1)
        def _():
            for c in range(2):
                t_ref[c] = e_new[c]

        @pl.when(ph == 0)
        def _():
            for stage in range(4):
                prepare(other, stage)
            prepare(h, 3)

        def unpack(n):
            m = rbuf[ph, n]
            w = roll(m, half)
            return jnp.where(low, m, w), jnp.where(low, w, m)

        sends[1].wait()
        sends[2].wait()
        got_b = unpack(2)
        for c in range(2):
            rs[other, c] += jnp.where(z_first, roll(got_b[c], plane), 0.0)

        @pl.when(h == 0)
        def _():
            sends[0].wait()
            got_t = unpack(0)
            for c in range(2):
                t_ref[c] = got_t[c]

        got_e = unpack(1)
        inputs = []
        for c in range(2):
            zin = jnp.where(z_last, roll(got_e[c], -plane), 0.0)
            inputs.append(jnp.where(first, zin, t_ref[c]))
        slot = lax.rem(ph, MR_MAX)
        put_operands(slot, 0, inputs[0], inputs[1])
        forward(slot, 1, lambda o, group, t: gh[other, o, 16 * t : 16 * t + 16, :])
        for c in range(2):
            u = gathered(c)
            rs[other, c] += u + roll(u, half)

        @pl.when(h == 1)
        def _():
            sends[0].wait()
            got_t = unpack(0)
            for c in range(2):
                rs[0, c] += got_t[c]

        return token

    lax.fori_loop(0, PHASES, phase, 0)

    for c in range(2):
        x_ref[c] = jnp.where(low, xs[0, c], xs[1, c])
        r_ref[c] = jnp.where(low, rs[0, c], rs[1, c])


def shards(nt, nz, rhs, links, clover, mr_steps):
    dof, lanes = rhs.shape[2], rhs.shape[-1]
    vmem = pl.BlockSpec(memory_space=pltpu.VMEM)
    hbm = pl.BlockSpec(memory_space=pltpu.HBM)
    operands = 3 * (dof // 16) + 2
    field = pltpu.VMEM((2, dof, lanes), F32)
    fields = pltpu.VMEM((2, 2, dof, lanes), F32)
    x, r = pl.pallas_call(
        functools.partial(kernel, nt, nz),
        out_shape=[jax.ShapeDtypeStruct((2, dof, lanes), F32)] * 2,
        in_specs=[hbm, hbm, hbm, hbm],
        out_specs=[vmem, vmem],
        scratch_shapes=[
            field,
            pltpu.SMEM((2,), jnp.int32),
            pltpu.VMEM((4, 2, dof, dof, lanes), BF16),
            pltpu.VMEM((2, dof, dof, lanes), BF16),
            pltpu.VMEM((2, dof, 4 * dof, lanes), BF16),
            pltpu.VMEM((2, dof, 4 * dof, lanes), BF16),
            pltpu.VMEM((2, dof, 2 * dof, lanes), BF16),
            pltpu.VMEM((2, dof, dof, lanes), BF16),
            fields,
            fields,
            field,
            field,
            field,
            field,
            fields,
            fields,
            field,
            pltpu.VMEM((6, dof, lanes), F32),
            pltpu.VMEM((MR_MAX, 2, 2, operands, 16, lanes), BF16),
            pltpu.VMEM((MR_MAX, 6, dof, 16, lanes), BF16),
            pltpu.VMEM((2, 8 * dof, lanes), F32),
            pltpu.VMEM((PHASES, 3, dof, lanes), F32),
            pltpu.VMEM((PHASES, 3, dof, lanes), F32),
            pltpu.SemaphoreType.DMA((7,)),
            pltpu.SemaphoreType.DMA((PHASES, 3)),
            pltpu.SemaphoreType.DMA((PHASES, 3)),
        ],
        compiler_params=pltpu.CompilerParams(
            collective_id=0, has_side_effects=True, vmem_limit_bytes=67043328
        ),
    )(
        rhs.reshape(2, dof, lanes),
        links.reshape(4, 2, dof, dof, lanes),
        clover.reshape(2, dof, dof, lanes),
        mr_steps.reshape(2),
    )
    return x.reshape(rhs.shape), r.reshape(rhs.shape)


def solution(mesh):
    placed = (
        P(None, None, None, "ta", "sa", None),
        P(None, None, None, None, "ta", "sa", None),
        P(None, None, None, "ta", "sa", None),
        P("ta", "sa", None),
    )
    return jax.shard_map(
        functools.partial(shards, mesh.shape["ta"], mesh.shape["sa"]),
        mesh=mesh,
        in_specs=placed,
        out_specs=(P(None, None, None, "ta", "sa", None), P(None, None, None, "ta", "sa", None)),
        check_vma=False,
    )
```

```python
import functools

import jax
import jax.numpy as jnp
from jax import lax
from jax.experimental import pallas as pl
from jax.experimental.pallas import tpu as pltpu
from jax.sharding import PartitionSpec as P

LZ = 4
LY = 4
LX = 4
MR_MAX = 3
SWEEPS = 2
PHASES = 2 * SWEEPS
PREPARE_UNROLL = 20
MESH = pl.DeviceIdType.MESH
F32 = jnp.float32
BF16 = jnp.bfloat16


def rows_of(dof):
    whole = dof // 16
    return [(16 * t, 16) for t in range(whole)] + [(16 * whole, dof - 16 * whole)]


def kernel(
    nt,
    nz,
    rhs_hbm,
    links_ref,
    clover_ref,
    steps_hbm,
    x_ref,
    r_ref,
    rhs_ref,
    steps_ref,
    lk,
    cl,
    gf,
    gb,
    gh,
    xr,
    rs,
    xs,
    q_ref,
    s_ref,
    e_ref,
    bs_ref,
    acc,
    bm_ref,
    t_ref,
    z_ref,
    gv,
    opf,
    pk,
    f_ref,
    sbuf,
    rbuf,
    csem,
    ssem,
    rsem,
):
    dof, lanes = rhs_ref.shape[1:]
    half = lanes // 2
    tiles = dof // 8
    whole = dof // 16
    packed = 2 * dof // 16
    pieces = rows_of(dof)
    ta = lax.axis_index("ta")
    sa = lax.axis_index("sa")
    t_next, t_prev = lax.rem(ta + 1, nt), lax.rem(ta + nt - 1, nt)
    z_next, z_prev = lax.rem(sa + 1, nz), lax.rem(sa + nz - 1, nz)

    copies = [
        pltpu.make_async_copy(links_ref.at[d], lk.at[d], csem.at[d]) for d in range(4)
    ] + [
        pltpu.make_async_copy(clover_ref, cl, csem.at[4]),
        pltpu.make_async_copy(rhs_hbm, rhs_ref, csem.at[5]),
        pltpu.make_async_copy(steps_hbm, steps_ref, csem.at[6]),
    ]
    for d in (5, 6, 1, 2, 3, 4, 0):
        copies[d].start()

    barrier = pltpu.get_barrier_semaphore()
    for where_to in ({"ta": t_next}, {"ta": t_prev}, {"sa": z_next}, {"sa": z_prev}):
        pl.semaphore_signal(barrier, inc=1, device_id=where_to, device_id_type=MESH)

    shape = (dof, lanes)
    lane = lax.broadcasted_iota(jnp.int32, shape, 1)
    row = lax.broadcasted_iota(jnp.int32, shape, 0)
    signs = jnp.where(row < dof // 2, 1.0, -1.0).astype(F32)
    low = lane < half
    site = lane % half
    zpos = site // (LY * LX)
    ypos = site // LX % LY
    xpos = site % LX
    z_last, z_first = zpos == LZ - 1, zpos == 0
    y_last, y_first = ypos == LY - 1, ypos == 0
    x_last, x_first = xpos == LX - 1, xpos == 0
    zero = jnp.zeros(shape, F32)
    plane = LY * LX

    def roll(v, by):
        return pltpu.roll(v, by % lanes, 1)

    def first_rows(h, rows):
        at = lax.broadcasted_iota(jnp.int32, (rows, lanes), 1)
        return jnp.where((at >= half) == ((at * 0 + h) == 1), 1.0, 0.0).astype(BF16) > 0.5

    def loop(body):
        def block(outer, carry):
            for inner in range(PREPARE_UNROLL):
                body(outer * PREPARE_UNROLL + inner)
            return carry

        lax.fori_loop(0, dof // PREPARE_UNROLL, block, 0)

    def prepare(h, stage):
        masks = {rows: first_rows(h, rows) for _, rows in pieces}

        def store(ref, i, base, top, c, at, rows, value):
            if rows == 16:
                ref[h, i, base + 16 * whole * c + at : base + 16 * whole * c + at + 16, :] = value
            else:
                ref[h, i, base + 32 * whole + 8 * c : base + 32 * whole + 8 * c + 8, :] = value

        def body(i):
            for c in range(2):
                for at, rows in pieces:
                    cut = slice(at, at + rows)
                    first = masks[rows]
                    if stage == 0:
                        z = pltpu.roll(lk[1, c, i, cut, :], half, 1)
                        g = jnp.where(first, lk[2, c, i, cut, :], z)
                        store(gf, i, 0, 0, c, at, rows, g)
                        store(gb, i, 2 * dof * c, 0, 0, at, rows, g)
                    if stage == 1:
                        x = pltpu.roll(lk[3, c, i, cut, :], half, 1)
                        xr[c, i, cut, :] = x
                        store(gf, i, 2 * dof, 0, c, at, rows, jnp.where(first, cl[c, i, cut, :], x))
                    if stage == 2:
                        g = jnp.where(first, lk[0, c, i, cut, :], xr[c, i, cut, :])
                        store(gb, i, 2 * dof * c, 0, 1, at, rows, g)
                    if stage == 3:
                        z = pltpu.roll(lk[1, c, i, cut, :], half, 1)
                        store(gh, i, 0, 0, c, at, rows, jnp.where(first, lk[0, c, i, cut, :], z))

        loop(body)

    copies[5].wait()
    for c in range(2):
        v = rhs_ref[c]
        w = roll(v, half)
        rs[0, c] = jnp.where(low, v, w)
        rs[1, c] = jnp.where(low, w, v)
        xs[0, c] = zero
        xs[1, c] = zero

    for stage, needs in enumerate(((1, 2), (3, 4), (0, 6))):
        for d in needs:
            copies[d].wait()
        prepare(sa % 2, stage)

    def fold(v):
        total = v[0:8]
        for t in range(1, tiles):
            total = total + v[8 * t : 8 * t + 8]
        return total

    def gathered(slot, part):
        parts = []
        for t in range(tiles):
            total = None
            for k in range(8):
                piece = f_ref[slot, part, pl.ds(8 * 8 * t + k, 8, stride=8), :]
                total = piece if total is None else total + piece
            parts.append(total)
        return jnp.concatenate(parts, axis=0)

    def two(v):
        high = v.astype(BF16).astype(F32)
        return high, v - high

    def put_operands(slot, group, vr, vi):
        for term, (r, i) in enumerate(zip(two(vr), two(vi))):
            n = -i
            top = 16 * whole
            out = [r[16 * t : 16 * t + 16] for t in range(whole)]
            out += [i[16 * t : 16 * t + 16] for t in range(whole)]
            out += [n[16 * t : 16 * t + 16] for t in range(whole)]
            out += [jnp.concatenate([r[top:], n[top:]], axis=0), jnp.concatenate([i[top:], r[top:]], axis=0)]
            for at, value in enumerate(out):
                opf[slot, group, term, at] = value.astype(BF16)

    def forward(slot, groups, matrix):
        def operand(group, term, at):
            return opf[slot, group, term, at].astype(F32)

        real = list(range(whole)) + list(range(2 * whole, 3 * whole)) + [3 * whole]
        imag = list(range(whole, 2 * whole)) + list(range(whole)) + [3 * whole + 1]
        for o in range(dof):
            sums = [None, None]
            for group in range(groups):
                for t in range(packed):
                    m = matrix(o, group, t).astype(F32)
                    for term in range(2):
                        for part, order in enumerate((real, imag)):
                            p = m * operand(group, term, order[t])
                            sums[part] = p if sums[part] is None else sums[part] + p
            for part in range(2):
                f_ref[slot, part, 8 * o : 8 * o + 8, :] = sums[part][0:8] + sums[part][8:16]

    def backward(slot, k, matrix):
        rounds = []
        t = 0
        while t + 1 < packed:
            rounds.append([(t, 0, dof), (t + 1, 0, dof)])
            t += 2
        if t < packed:
            rounds.append([(t, 0, dof // 2), (t, dof // 2, dof)])
        done = {}
        for index, chains in enumerate(rounds):
            sums = [[None, None] for _ in chains]
            for step in range(chains[0][2] - chains[0][1]):
                if index == 0:
                    for n in range(6):
                        spread = jnp.broadcast_to(gv[k, n, pl.ds(step, 1), :], (16, lanes))
                        pk[slot, n, step] = spread.astype(BF16)
                for chain, (t, start, _) in enumerate(chains):
                    i = start + step
                    mr = matrix(i, 0, t).astype(F32)
                    mi = matrix(i, 1, t).astype(F32)
                    x = [pk[slot, n, i].astype(F32) for n in range(6)]
                    for part, terms in enumerate(
                        (
                            ((mr, x[0]), (mr, x[1]), (mi, x[2]), (mi, x[3])),
                            ((mr, x[2]), (mr, x[3]), (mi, x[4]), (mi, x[5])),
                        )
                    ):
                        for m, y in terms:
                            p = m * y
                            old = sums[chain][part]
                            sums[chain][part] = p if old is None else old + p
            for chain, (t, _, _) in enumerate(chains):
                if t in done:
                    done[t] = [a + b for a, b in zip(done[t], sums[chain])]
                else:
                    done[t] = sums[chain]
        out = []
        for group in range(2):
            out.append([])
            for part in range(2):
                parts = [done[whole * group + t][part] for t in range(whole)]
                parts.append(done[2 * whole][part][8 * group : 8 * group + 8])
                out[group].append(-signs * jnp.concatenate(parts, axis=0))
        return out

    def phase(ph, token):
        h = lax.rem(ph + sa, 2)
        other = 1 - h
        limit = steps_ref[h]
        first = (lane >= half) == ((lane * 0 + h) == 1)
        h_is_0 = (lane * 0 + h) == 0

        def ahead(v):
            n = -v
            ya = jnp.where(y_last, roll(n, (LY - 1) * LX), roll(n, -LX))
            za = jnp.where(z_last, 0.0, roll(n, -plane))
            xa = jnp.where(x_last, roll(n, LX - 1), roll(n, -1))
            return jnp.where(first, ya, za), jnp.where(first, v, xa)

        def total(v):
            return jnp.sum(jnp.sum(fold(v), axis=0, keepdims=True), axis=1, keepdims=True)

        def scale(k, q, s):
            numer_real = total(q[0] * s[0] + q[1] * s[1])
            numer_imag = total(q[0] * s[1] - q[1] * s[0])
            denom = total(q[0] * q[0] + q[1] * q[1]) + 2e-6
            live = (lane[0:1] * 0 + limit) > k
            ar = jnp.where(live, jnp.broadcast_to(numer_real / denom, (1, lanes)), 0.0)
            ai = jnp.where(live, jnp.broadcast_to(numer_imag / denom, (1, lanes)), 0.0)
            return ar, ai

        def times(a, v):
            return [a[0] * v[0] - a[1] * v[1], a[0] * v[1] + a[1] * v[0]]

        def plus(u, v):
            return [u[0] + v[0], u[1] + v[1]]

        def minus(u, v):
            return [u[0] - v[0], u[1] - v[1]]

        def keep(ref, v):
            for c in range(2):
                ref[c] = v[c]

        def kept(ref):
            return [ref[0], ref[1]]

        def apply(k, v):
            slot = lax.rem(ph + k, MR_MAX)
            gr, gi = two(signs * v[0]), two(signs * v[1])
            for term in range(2):
                gv[k, term] = gr[term]
                gv[k, 2 + term] = gi[term]
                gv[k, 4 + term] = -gr[term]
            aheads = [ahead(v[0]), ahead(v[1])]
            for group in range(2):
                put_operands(slot, group, aheads[0][group], aheads[1][group])
            back0, back2 = backward(
                slot,
                k,
                lambda i, c, t: gb[h, i, 2 * dof * c + 16 * t : 2 * dof * c + 16 * t + 16, :],
            )
            near = []
            for c in range(2):
                b, d = back0[c], back2[c]
                yb = jnp.where(y_first, roll(b, -(LY - 1) * LX), roll(b, LX))
                zb = jnp.where(z_first, 0.0, roll(b, plane))
                xb = jnp.where(x_first, roll(d, -(LX - 1)), roll(d, 1))
                u = jnp.where(first, yb, zb) + jnp.where(first, 0.0, xb)
                near.append(u + roll(u, half))
                bm_ref[k, 0, c] = jnp.where(first, roll(b, half), b)
                bm_ref[k, 1, c] = jnp.where(first, d, roll(d, half))
            forward(
                slot,
                2,
                lambda o, group, t: gf[h, o, 2 * dof * group + 16 * t : 2 * dof * group + 16 * t + 16, :],
            )
            out = []
            for c in range(2):
                u = gathered(slot, c)
                out.append(u + roll(u, half) + near[c])
            return out

        s = kept(rs.at[h])
        q = apply(0, s)
        alpha = scale(0, q, s)
        w = apply(1, q)
        e = times(alpha, s)
        s = minus(s, times(alpha, q))
        q = minus(q, times(alpha, w))
        keep(e_ref, e)
        keep(s_ref, s)
        keep(q_ref, q)
        for n in range(2):
            b = kept(bm_ref.at[0, n])
            keep(acc.at[n], times(alpha, b))
            keep(bs_ref.at[n], minus(b, times(alpha, kept(bm_ref.at[1, n]))))
        alpha = scale(1, q, s)
        w = apply(2, q)
        s, q = kept(s_ref), kept(q_ref)
        e = plus(kept(e_ref), times(alpha, s))
        s = minus(s, times(alpha, q))
        q = minus(q, times(alpha, w))
        back = []
        for n in range(2):
            b = kept(bs_ref.at[n])
            total_b = plus(kept(acc.at[n]), times(alpha, b))
            back.append((total_b, minus(b, times(alpha, kept(bm_ref.at[2, n])))))

        def pack(v):
            return jnp.where(low, v[0], v[1])

        def sender(n, where_to, src, dst):
            return pltpu.make_async_remote_copy(
                src_ref=src,
                dst_ref=dst,
                send_sem=ssem.at[ph, n],
                recv_sem=rsem.at[ph, n],
                device_id=where_to,
                device_id_type=MESH,
            )

        target = {"ta": lax.rem(ta + nt + 2 * h - 1, nt)}

        @pl.when(ph == 0)
        def _():
            pl.semaphore_wait(barrier, 4)

        alpha = scale(2, q, s)
        e_new = plus(e, times(alpha, s))
        bt = [-v for v in plus(back[1][0], times(alpha, back[1][1]))]
        sbuf[ph, 0] = jnp.where(h_is_0, pack(e_new), pack(bt))
        sends = [sender(0, target, sbuf.at[ph, 0], rbuf.at[ph, 0])]
        sends[0].start()
        bz = [-v for v in plus(back[0][0], times(alpha, back[0][1]))]
        sbuf[ph, 1] = pack(e_new)
        sbuf[ph, 2] = pack(bz)
        sends.append(sender(1, {"sa": z_prev}, sbuf.at[ph, 1], rbuf.at[ph, 1]))
        sends.append(sender(2, {"sa": z_next}, sbuf.at[ph, 2], rbuf.at[ph, 2]))
        sends[1].start()
        sends[2].start()

        left = minus(s, times(alpha, q))
        for c in range(2):
            xs[h, c] += e_new[c]
            rs[h, c] = left[c]

        @pl.when(h == 0)
        def _():
            for c in range(2):
                rs[1, c] += bt[c]

        @pl.when(h == 1)
        def _():
            for c in range(2):
                t_ref[c] = e_new[c]

        @pl.when(ph == 0)
        def _():
            for stage in range(4):
                prepare(other, stage)
            prepare(h, 3)

        def unpack(n):
            m = rbuf[ph, n]
            w = roll(m, half)
            return jnp.where(low, m, w), jnp.where(low, w, m)

        sends[1].wait()
        sends[2].wait()
        m = rbuf[ph, 2]
        near_low, near_high = roll(m, half + plane), roll(m, plane)
        rs[other, 0] += jnp.where(z_first, jnp.where(low, near_low, near_high), 0.0)
        rs[other, 1] += jnp.where(z_first, jnp.where(low, near_high, near_low), 0.0)
        m = rbuf[ph, 1]
        own, far = roll(m, half - plane), roll(m, -plane)
        zin = (
            jnp.where(z_last, jnp.where(h_is_0, own, far), 0.0),
            jnp.where(z_last, jnp.where(h_is_0, far, own), 0.0),
        )
        for c in range(2):
            z_ref[c] = zin[c]

        @pl.when(h == 0)
        def _():
            sends[0].wait()
            m = rbuf[ph, 0]
            t_ref[0] = roll(m, half)
            t_ref[1] = m

        inputs = [jnp.where(first, z_ref[c], t_ref[c]) for c in range(2)]
        slot = lax.rem(ph, MR_MAX)
        put_operands(slot, 0, inputs[0], inputs[1])
        forward(slot, 1, lambda o, group, t: gh[other, o, 16 * t : 16 * t + 16, :])
        for c in range(2):
            u = gathered(slot, c)
            rs[other, c] += u + roll(u, half)

        @pl.when(h == 1)
        def _():
            sends[0].wait()
            got_t = unpack(0)
            for c in range(2):
                rs[0, c] += got_t[c]

        return token

    lax.fori_loop(0, PHASES, phase, 0)

    for c in range(2):
        x_ref[c] = jnp.where(low, xs[0, c], xs[1, c])
        r_ref[c] = jnp.where(low, rs[0, c], rs[1, c])


def shards(nt, nz, rhs, links, clover, mr_steps):
    dof, lanes = rhs.shape[2], rhs.shape[-1]
    vmem = pl.BlockSpec(memory_space=pltpu.VMEM)
    hbm = pl.BlockSpec(memory_space=pltpu.HBM)
    operands = 3 * (dof // 16) + 2
    field = pltpu.VMEM((2, dof, lanes), F32)
    fields = pltpu.VMEM((2, 2, dof, lanes), F32)
    x, r = pl.pallas_call(
        functools.partial(kernel, nt, nz),
        out_shape=[jax.ShapeDtypeStruct((2, dof, lanes), F32)] * 2,
        in_specs=[hbm, hbm, hbm, hbm],
        out_specs=[vmem, vmem],
        scratch_shapes=[
            field,
            pltpu.SMEM((2,), jnp.int32),
            pltpu.VMEM((4, 2, dof, dof, lanes), BF16),
            pltpu.VMEM((2, dof, dof, lanes), BF16),
            pltpu.VMEM((2, dof, 4 * dof, lanes), BF16),
            pltpu.VMEM((2, dof, 4 * dof, lanes), BF16),
            pltpu.VMEM((2, dof, 2 * dof, lanes), BF16),
            pltpu.VMEM((2, dof, dof, lanes), BF16),
            fields,
            fields,
            field,
            field,
            field,
            fields,
            fields,
            pltpu.VMEM((MR_MAX, 2, 2, dof, lanes), F32),
            field,
            field,
            pltpu.VMEM((MR_MAX, 6, dof, lanes), F32),
            pltpu.VMEM((MR_MAX, 2, 2, operands, 16, lanes), BF16),
            pltpu.VMEM((MR_MAX, 6, dof, 16, lanes), BF16),
            pltpu.VMEM((MR_MAX, 2, 8 * dof, lanes), F32),
            pltpu.VMEM((PHASES, 3, dof, lanes), F32),
            pltpu.VMEM((PHASES, 3, dof, lanes), F32),
            pltpu.SemaphoreType.DMA((7,)),
            pltpu.SemaphoreType.DMA((PHASES, 3)),
            pltpu.SemaphoreType.DMA((PHASES, 3)),
        ],
        compiler_params=pltpu.CompilerParams(
            collective_id=0, has_side_effects=True, vmem_limit_bytes=67043328
        ),
    )(
        rhs.reshape(2, dof, lanes),
        links.reshape(4, 2, dof, dof, lanes),
        clover.reshape(2, dof, dof, lanes),
        mr_steps.reshape(2),
    )
    return x.reshape(rhs.shape), r.reshape(rhs.shape)


def solution(mesh):
    placed = (
        P(None, None, None, "ta", "sa", None),
        P(None, None, None, None, "ta", "sa", None),
        P(None, None, None, "ta", "sa", None),
        P("ta", "sa", None),
    )
    return jax.shard_map(
        functools.partial(shards, mesh.shape["ta"], mesh.shape["sa"]),
        mesh=mesh,
        in_specs=placed,
        out_specs=(P(None, None, None, "ta", "sa", None), P(None, None, None, "ta", "sa", None)),
        check_vma=False,
    )
```

```python
import functools

import jax
import jax.numpy as jnp
from jax import lax
from jax.experimental import pallas as pl
from jax.experimental.pallas import tpu as pltpu
from jax.sharding import PartitionSpec as P

LZ = 4
LY = 4
LX = 4
MR_MAX = 3
SWEEPS = 2
PHASES = 2 * SWEEPS
PREPARE_UNROLL = 20
MESH = pl.DeviceIdType.MESH
F32 = jnp.float32
BF16 = jnp.bfloat16


def rows_of(dof):
    whole = dof // 16
    return [(16 * t, 16) for t in range(whole)] + [(16 * whole, dof - 16 * whole)]


def kernel(
    nt,
    nz,
    rhs_hbm,
    links_ref,
    clover_ref,
    steps_hbm,
    out_ref,
    rhs_ref,
    steps_ref,
    lk,
    cl,
    gf,
    gb,
    gh,
    xr,
    rs,
    xs,
    q_ref,
    s_ref,
    e_ref,
    bs_ref,
    acc,
    bm_ref,
    t_ref,
    z_ref,
    gv,
    opf,
    pk,
    f_ref,
    sbuf,
    rbuf,
    csem,
    ssem,
    rsem,
):
    dof, lanes = rhs_ref.shape[1:]
    half = lanes // 2
    tiles = dof // 8
    whole = dof // 16
    packed = 2 * dof // 16
    pieces = rows_of(dof)
    ta = lax.axis_index("ta")
    sa = lax.axis_index("sa")
    t_next, t_prev = lax.rem(ta + 1, nt), lax.rem(ta + nt - 1, nt)
    z_next, z_prev = lax.rem(sa + 1, nz), lax.rem(sa + nz - 1, nz)

    copies = [
        pltpu.make_async_copy(links_ref.at[d], lk.at[d], csem.at[d]) for d in range(4)
    ] + [
        pltpu.make_async_copy(clover_ref, cl, csem.at[4]),
        pltpu.make_async_copy(rhs_hbm, rhs_ref, csem.at[5]),
        pltpu.make_async_copy(steps_hbm, steps_ref, csem.at[6]),
    ]
    for d in (5, 6, 1, 2, 3, 4, 0):
        copies[d].start()

    barrier = pltpu.get_barrier_semaphore()
    for where_to in ({"ta": t_next}, {"ta": t_prev}, {"sa": z_next}, {"sa": z_prev}):
        pl.semaphore_signal(barrier, inc=1, device_id=where_to, device_id_type=MESH)

    shape = (dof, lanes)
    lane = lax.broadcasted_iota(jnp.int32, shape, 1)
    row = lax.broadcasted_iota(jnp.int32, shape, 0)
    signs = jnp.where(row < dof // 2, 1.0, -1.0).astype(F32)
    low = lane < half
    site = lane % half
    zpos = site // (LY * LX)
    ypos = site // LX % LY
    xpos = site % LX
    z_last, z_first = zpos == LZ - 1, zpos == 0
    y_last, y_first = ypos == LY - 1, ypos == 0
    x_last, x_first = xpos == LX - 1, xpos == 0
    zero = jnp.zeros(shape, F32)
    plane = LY * LX

    def roll(v, by):
        return pltpu.roll(v, by % lanes, 1)

    def first_rows(h, rows):
        at = lax.broadcasted_iota(jnp.int32, (rows, lanes), 1)
        return jnp.where((at >= half) == ((at * 0 + h) == 1), 1.0, 0.0).astype(BF16) > 0.5

    def loop(body):
        def block(outer, carry):
            for inner in range(PREPARE_UNROLL):
                body(outer * PREPARE_UNROLL + inner)
            return carry

        lax.fori_loop(0, dof // PREPARE_UNROLL, block, 0)

    def prepare(h, stage):
        masks = {rows: first_rows(h, rows) for _, rows in pieces}

        def store(ref, i, base, top, c, at, rows, value):
            if rows == 16:
                ref[h, i, base + 16 * whole * c + at : base + 16 * whole * c + at + 16, :] = value
            else:
                ref[h, i, base + 32 * whole + 8 * c : base + 32 * whole + 8 * c + 8, :] = value

        def body(i):
            for c in range(2):
                for at, rows in pieces:
                    cut = slice(at, at + rows)
                    first = masks[rows]
                    if stage == 0:
                        z = pltpu.roll(lk[1, c, i, cut, :], half, 1)
                        g = jnp.where(first, lk[2, c, i, cut, :], z)
                        store(gf, i, 0, 0, c, at, rows, g)
                        store(gb, i, 2 * dof * c, 0, 0, at, rows, g)
                    if stage == 1:
                        x = pltpu.roll(lk[3, c, i, cut, :], half, 1)
                        xr[c, i, cut, :] = x
                        store(gf, i, 2 * dof, 0, c, at, rows, jnp.where(first, cl[c, i, cut, :], x))
                    if stage == 2:
                        g = jnp.where(first, lk[0, c, i, cut, :], xr[c, i, cut, :])
                        store(gb, i, 2 * dof * c, 0, 1, at, rows, g)
                    if stage == 3:
                        z = pltpu.roll(lk[1, c, i, cut, :], half, 1)
                        store(gh, i, 0, 0, c, at, rows, jnp.where(first, lk[0, c, i, cut, :], z))

        loop(body)

    copies[5].wait()
    for c in range(2):
        v = rhs_ref[c]
        w = roll(v, half)
        rs[0, c] = jnp.where(low, v, w)
        rs[1, c] = jnp.where(low, w, v)
        xs[0, c] = zero
        xs[1, c] = zero

    for stage, needs in enumerate(((1, 2), (3, 4), (0, 6))):
        for d in needs:
            copies[d].wait()
        prepare(sa % 2, stage)

    def fold(v):
        total = v[0:8]
        for t in range(1, tiles):
            total = total + v[8 * t : 8 * t + 8]
        return total

    def gathered(slot, part):
        parts = []
        for t in range(tiles):
            total = None
            for k in range(8):
                piece = f_ref[slot, part, pl.ds(8 * 8 * t + k, 8, stride=8), :]
                total = piece if total is None else total + piece
            parts.append(total)
        return jnp.concatenate(parts, axis=0)

    def two(v):
        high = v.astype(BF16).astype(F32)
        return high, v - high

    def put_operands(slot, group, vr, vi):
        for term, (r, i) in enumerate(zip(two(vr), two(vi))):
            n = -i
            top = 16 * whole
            out = [r[16 * t : 16 * t + 16] for t in range(whole)]
            out += [i[16 * t : 16 * t + 16] for t in range(whole)]
            out += [n[16 * t : 16 * t + 16] for t in range(whole)]
            out += [jnp.concatenate([r[top:], n[top:]], axis=0), jnp.concatenate([i[top:], r[top:]], axis=0)]
            for at, value in enumerate(out):
                opf[slot, group, term, at] = value.astype(BF16)

    def forward(slot, groups, matrix):
        def operand(group, term, at):
            return opf[slot, group, term, at].astype(F32)

        real = list(range(whole)) + list(range(2 * whole, 3 * whole)) + [3 * whole]
        imag = list(range(whole, 2 * whole)) + list(range(whole)) + [3 * whole + 1]
        for o in range(dof):
            sums = [None, None]
            for group in range(groups):
                for t in range(packed):
                    m = matrix(o, group, t).astype(F32)
                    for term in range(2):
                        for part, order in enumerate((real, imag)):
                            p = m * operand(group, term, order[t])
                            sums[part] = p if sums[part] is None else sums[part] + p
            for part in range(2):
                f_ref[slot, part, 8 * o : 8 * o + 8, :] = sums[part][0:8] + sums[part][8:16]

    def backward(slot, k, matrix):
        rounds = []
        t = 0
        while t + 1 < packed:
            rounds.append([(t, 0, dof), (t + 1, 0, dof)])
            t += 2
        if t < packed:
            rounds.append([(t, 0, dof // 2), (t, dof // 2, dof)])
        done = {}
        for index, chains in enumerate(rounds):
            sums = [[None, None] for _ in chains]
            for step in range(chains[0][2] - chains[0][1]):
                if index == 0:
                    for n in range(6):
                        spread = jnp.broadcast_to(gv[k, n, pl.ds(step, 1), :], (16, lanes))
                        pk[slot, n, step] = spread.astype(BF16)
                for chain, (t, start, _) in enumerate(chains):
                    i = start + step
                    mr = matrix(i, 0, t).astype(F32)
                    mi = matrix(i, 1, t).astype(F32)
                    x = [pk[slot, n, i].astype(F32) for n in range(6)]
                    for part, terms in enumerate(
                        (
                            ((mr, x[0]), (mr, x[1]), (mi, x[2]), (mi, x[3])),
                            ((mr, x[2]), (mr, x[3]), (mi, x[4]), (mi, x[5])),
                        )
                    ):
                        for m, y in terms:
                            p = m * y
                            old = sums[chain][part]
                            sums[chain][part] = p if old is None else old + p
            for chain, (t, _, _) in enumerate(chains):
                if t in done:
                    done[t] = [a + b for a, b in zip(done[t], sums[chain])]
                else:
                    done[t] = sums[chain]
        out = []
        for group in range(2):
            out.append([])
            for part in range(2):
                parts = [done[whole * group + t][part] for t in range(whole)]
                parts.append(done[2 * whole][part][8 * group : 8 * group + 8])
                out[group].append(-signs * jnp.concatenate(parts, axis=0))
        return out

    def phase(ph, token):
        h = lax.rem(ph + sa, 2)
        other = 1 - h
        limit = steps_ref[h]
        first = (lane >= half) == ((lane * 0 + h) == 1)
        h_is_0 = (lane * 0 + h) == 0

        def ahead(v):
            n = -v
            ya = jnp.where(y_last, roll(n, (LY - 1) * LX), roll(n, -LX))
            za = jnp.where(z_last, 0.0, roll(n, -plane))
            xa = jnp.where(x_last, roll(n, LX - 1), roll(n, -1))
            return jnp.where(first, ya, za), jnp.where(first, v, xa)

        def total(v):
            return jnp.sum(jnp.sum(fold(v), axis=0, keepdims=True), axis=1, keepdims=True)

        def scale(k, q, s):
            numer_real = total(q[0] * s[0] + q[1] * s[1])
            numer_imag = total(q[0] * s[1] - q[1] * s[0])
            denom = total(q[0] * q[0] + q[1] * q[1]) + 2e-6
            live = (lane[0:1] * 0 + limit) > k
            ar = jnp.where(live, jnp.broadcast_to(numer_real / denom, (1, lanes)), 0.0)
            ai = jnp.where(live, jnp.broadcast_to(numer_imag / denom, (1, lanes)), 0.0)
            return ar, ai

        def times(a, v):
            return [a[0] * v[0] - a[1] * v[1], a[0] * v[1] + a[1] * v[0]]

        def plus(u, v):
            return [u[0] + v[0], u[1] + v[1]]

        def minus(u, v):
            return [u[0] - v[0], u[1] - v[1]]

        def keep(ref, v):
            for c in range(2):
                ref[c] = v[c]

        def kept(ref):
            return [ref[0], ref[1]]

        def apply(k, v):
            slot = lax.rem(ph + k, MR_MAX)
            gr, gi = two(signs * v[0]), two(signs * v[1])
            for term in range(2):
                gv[k, term] = gr[term]
                gv[k, 2 + term] = gi[term]
                gv[k, 4 + term] = -gr[term]
            aheads = [ahead(v[0]), ahead(v[1])]
            for group in range(2):
                put_operands(slot, group, aheads[0][group], aheads[1][group])
            back0, back2 = backward(
                slot,
                k,
                lambda i, c, t: gb[h, i, 2 * dof * c + 16 * t : 2 * dof * c + 16 * t + 16, :],
            )
            near = []
            for c in range(2):
                b, d = back0[c], back2[c]
                yb = jnp.where(y_first, roll(b, -(LY - 1) * LX), roll(b, LX))
                zb = jnp.where(z_first, 0.0, roll(b, plane))
                xb = jnp.where(x_first, roll(d, -(LX - 1)), roll(d, 1))
                u = jnp.where(first, yb, zb) + jnp.where(first, 0.0, xb)
                near.append(u + roll(u, half))
                bm_ref[k, 0, c] = jnp.where(first, roll(b, half), b)
                bm_ref[k, 1, c] = jnp.where(first, d, roll(d, half))
            forward(
                slot,
                2,
                lambda o, group, t: gf[h, o, 2 * dof * group + 16 * t : 2 * dof * group + 16 * t + 16, :],
            )
            out = []
            for c in range(2):
                u = gathered(slot, c)
                out.append(u + roll(u, half) + near[c])
            return out

        s = kept(rs.at[h])
        q = apply(0, s)
        alpha = scale(0, q, s)
        w = apply(1, q)
        e = times(alpha, s)
        s = minus(s, times(alpha, q))
        q = minus(q, times(alpha, w))
        keep(e_ref, e)
        keep(s_ref, s)
        keep(q_ref, q)
        for n in range(2):
            b = kept(bm_ref.at[0, n])
            keep(acc.at[n], times(alpha, b))
            keep(bs_ref.at[n], minus(b, times(alpha, kept(bm_ref.at[1, n]))))
        alpha = scale(1, q, s)
        w = apply(2, q)
        s, q = kept(s_ref), kept(q_ref)
        e = plus(kept(e_ref), times(alpha, s))
        s = minus(s, times(alpha, q))
        q = minus(q, times(alpha, w))
        back = []
        for n in range(2):
            b = kept(bs_ref.at[n])
            total_b = plus(kept(acc.at[n]), times(alpha, b))
            back.append((total_b, minus(b, times(alpha, kept(bm_ref.at[2, n])))))

        def pack(v):
            return jnp.where(low, v[0], v[1])

        def sender(n, where_to, src, dst):
            return pltpu.make_async_remote_copy(
                src_ref=src,
                dst_ref=dst,
                send_sem=ssem.at[ph, n],
                recv_sem=rsem.at[ph, n],
                device_id=where_to,
                device_id_type=MESH,
            )

        target = {"ta": lax.rem(ta + nt + 2 * h - 1, nt)}

        @pl.when(ph == 0)
        def _():
            pl.semaphore_wait(barrier, 4)

        alpha = scale(2, q, s)
        e_new = plus(e, times(alpha, s))
        bt = [-v for v in plus(back[1][0], times(alpha, back[1][1]))]
        sbuf[ph, 0] = jnp.where(h_is_0, pack(e_new), pack(bt))
        sends = [sender(0, target, sbuf.at[ph, 0], rbuf.at[ph, 0])]
        sends[0].start()
        bz = [-v for v in plus(back[0][0], times(alpha, back[0][1]))]
        sbuf[ph, 1] = pack(e_new)
        sbuf[ph, 2] = pack(bz)
        sends.append(sender(1, {"sa": z_prev}, sbuf.at[ph, 1], rbuf.at[ph, 1]))
        sends.append(sender(2, {"sa": z_next}, sbuf.at[ph, 2], rbuf.at[ph, 2]))
        sends[1].start()
        sends[2].start()

        left = minus(s, times(alpha, q))
        for c in range(2):
            xs[h, c] += e_new[c]
            rs[h, c] = left[c]

        @pl.when(h == 0)
        def _():
            for c in range(2):
                rs[1, c] += bt[c]

        @pl.when(h == 1)
        def _():
            for c in range(2):
                t_ref[c] = e_new[c]

        @pl.when(ph == 0)
        def _():
            for stage in range(4):
                prepare(other, stage)
            prepare(h, 3)

        def unpack(n):
            m = rbuf[ph, n]
            w = roll(m, half)
            return jnp.where(low, m, w), jnp.where(low, w, m)

        sends[1].wait()
        sends[2].wait()
        m = rbuf[ph, 2]
        near_low, near_high = roll(m, half + plane), roll(m, plane)
        rs[other, 0] += jnp.where(z_first, jnp.where(low, near_low, near_high), 0.0)
        rs[other, 1] += jnp.where(z_first, jnp.where(low, near_high, near_low), 0.0)
        m = rbuf[ph, 1]
        own, far = roll(m, half - plane), roll(m, -plane)
        zin = (
            jnp.where(z_last, jnp.where(h_is_0, own, far), 0.0),
            jnp.where(z_last, jnp.where(h_is_0, far, own), 0.0),
        )
        for c in range(2):
            z_ref[c] = zin[c]

        @pl.when(h == 0)
        def _():
            sends[0].wait()
            m = rbuf[ph, 0]
            t_ref[0] = roll(m, half)
            t_ref[1] = m

        inputs = [jnp.where(first, z_ref[c], t_ref[c]) for c in range(2)]
        slot = lax.rem(ph, MR_MAX)
        put_operands(slot, 0, inputs[0], inputs[1])
        forward(slot, 1, lambda o, group, t: gh[other, o, 16 * t : 16 * t + 16, :])
        for c in range(2):
            u = gathered(slot, c)
            rs[other, c] += u + roll(u, half)

        @pl.when(h == 1)
        def _():
            sends[0].wait()
            got_t = unpack(0)
            for c in range(2):
                rs[0, c] += got_t[c]

        return token

    lax.fori_loop(0, PHASES, phase, 0)

    for c in range(2):
        out_ref[0, c] = jnp.where(low, xs[0, c], xs[1, c])
        out_ref[1, c] = jnp.where(low, rs[0, c], rs[1, c])


def shards(nt, nz, rhs, links, clover, mr_steps):
    dof, lanes = rhs.shape[2], rhs.shape[-1]
    vmem = pl.BlockSpec(memory_space=pltpu.VMEM)
    hbm = pl.BlockSpec(memory_space=pltpu.HBM)
    operands = 3 * (dof // 16) + 2
    field = pltpu.VMEM((2, dof, lanes), F32)
    fields = pltpu.VMEM((2, 2, dof, lanes), F32)
    out = pl.pallas_call(
        functools.partial(kernel, nt, nz),
        out_shape=jax.ShapeDtypeStruct((2, 2, dof, lanes), F32),
        in_specs=[hbm, hbm, hbm, hbm],
        out_specs=vmem,
        scratch_shapes=[
            field,
            pltpu.SMEM((2,), jnp.int32),
            pltpu.VMEM((4, 2, dof, dof, lanes), BF16),
            pltpu.VMEM((2, dof, dof, lanes), BF16),
            pltpu.VMEM((2, dof, 4 * dof, lanes), BF16),
            pltpu.VMEM((2, dof, 4 * dof, lanes), BF16),
            pltpu.VMEM((2, dof, 2 * dof, lanes), BF16),
            pltpu.VMEM((2, dof, dof, lanes), BF16),
            fields,
            fields,
            field,
            field,
            field,
            fields,
            fields,
            pltpu.VMEM((MR_MAX, 2, 2, dof, lanes), F32),
            field,
            field,
            pltpu.VMEM((MR_MAX, 6, dof, lanes), F32),
            pltpu.VMEM((MR_MAX, 2, 2, operands, 16, lanes), BF16),
            pltpu.VMEM((MR_MAX, 6, dof, 16, lanes), BF16),
            pltpu.VMEM((MR_MAX, 2, 8 * dof, lanes), F32),
            pltpu.VMEM((PHASES, 3, dof, lanes), F32),
            pltpu.VMEM((PHASES, 3, dof, lanes), F32),
            pltpu.SemaphoreType.DMA((7,)),
            pltpu.SemaphoreType.DMA((PHASES, 3)),
            pltpu.SemaphoreType.DMA((PHASES, 3)),
        ],
        compiler_params=pltpu.CompilerParams(
            collective_id=0, has_side_effects=True, vmem_limit_bytes=67043328
        ),
    )(
        rhs.reshape(2, dof, lanes),
        links.reshape(4, 2, dof, dof, lanes),
        clover.reshape(2, dof, dof, lanes),
        mr_steps.reshape(2),
    )
    return out[0].reshape(rhs.shape), out[1].reshape(rhs.shape)


def solution(mesh):
    placed = (
        P(None, None, None, "ta", "sa", None),
        P(None, None, None, None, "ta", "sa", None),
        P(None, None, None, "ta", "sa", None),
        P("ta", "sa", None),
    )
    return jax.shard_map(
        functools.partial(shards, mesh.shape["ta"], mesh.shape["sa"]),
        mesh=mesh,
        in_specs=placed,
        out_specs=(P(None, None, None, "ta", "sa", None), P(None, None, None, "ta", "sa", None)),
        check_vma=False,
    )
```

```python
import functools

import jax
import jax.numpy as jnp
from jax import lax
from jax.experimental import pallas as pl
from jax.experimental.pallas import tpu as pltpu
from jax.sharding import PartitionSpec as P

LZ = 4
LY = 4
LX = 4
MR_MAX = 3
SWEEPS = 2
PHASES = 2 * SWEEPS
PREPARE_UNROLL = 20
MESH = pl.DeviceIdType.MESH
F32 = jnp.float32
BF16 = jnp.bfloat16


def rows_of(dof):
    whole = dof // 16
    return [(16 * t, 16) for t in range(whole)] + [(16 * whole, dof - 16 * whole)]


def kernel(
    nt,
    nz,
    rhs_hbm,
    links_ref,
    clover_ref,
    steps_hbm,
    out_ref,
    rhs_ref,
    steps_ref,
    lk,
    cl,
    gf,
    gb,
    gh,
    xr,
    rs,
    xs,
    q_ref,
    s_ref,
    e_ref,
    bs_ref,
    acc,
    bm_ref,
    t_ref,
    z_ref,
    gv,
    opf,
    pk,
    f_ref,
    sbuf,
    rbuf,
    csem,
    ssem,
    rsem,
):
    dof, lanes = rhs_ref.shape[1:]
    half = lanes // 2
    tiles = dof // 8
    whole = dof // 16
    packed = 2 * dof // 16
    pieces = rows_of(dof)
    ta = lax.axis_index("ta")
    sa = lax.axis_index("sa")
    t_next, t_prev = lax.rem(ta + 1, nt), lax.rem(ta + nt - 1, nt)
    z_next, z_prev = lax.rem(sa + 1, nz), lax.rem(sa + nz - 1, nz)

    barrier = pltpu.get_barrier_semaphore()
    for where_to in ({"ta": t_next}, {"ta": t_prev}, {"sa": z_next}, {"sa": z_prev}):
        pl.semaphore_signal(barrier, inc=1, device_id=where_to, device_id_type=MESH)

    copies = [
        pltpu.make_async_copy(links_ref.at[d], lk.at[d], csem.at[d]) for d in range(4)
    ] + [
        pltpu.make_async_copy(clover_ref, cl, csem.at[4]),
        pltpu.make_async_copy(rhs_hbm, rhs_ref, csem.at[5]),
        pltpu.make_async_copy(steps_hbm, steps_ref, csem.at[6]),
    ]
    for d in (5, 6, 1, 2, 3, 4, 0):
        copies[d].start()

    shape = (dof, lanes)
    lane = lax.broadcasted_iota(jnp.int32, shape, 1)
    row = lax.broadcasted_iota(jnp.int32, shape, 0)
    signs = jnp.where(row < dof // 2, 1.0, -1.0).astype(F32)
    low = lane < half
    site = lane % half
    zpos = site // (LY * LX)
    ypos = site // LX % LY
    xpos = site % LX
    z_last, z_first = zpos == LZ - 1, zpos == 0
    y_last, y_first = ypos == LY - 1, ypos == 0
    x_last, x_first = xpos == LX - 1, xpos == 0
    zero = jnp.zeros(shape, F32)
    plane = LY * LX

    def roll(v, by):
        return pltpu.roll(v, by % lanes, 1)

    def first_rows(h, rows):
        at = lax.broadcasted_iota(jnp.int32, (rows, lanes), 1)
        return jnp.where((at >= half) == ((at * 0 + h) == 1), 1.0, 0.0).astype(BF16) > 0.5

    def loop(body):
        def block(outer, carry):
            for inner in range(PREPARE_UNROLL):
                body(outer * PREPARE_UNROLL + inner)
            return carry

        lax.fori_loop(0, dof // PREPARE_UNROLL, block, 0)

    def prepare(h, stage):
        masks = {rows: first_rows(h, rows) for _, rows in pieces}

        def store(ref, i, base, top, c, at, rows, value):
            if rows == 16:
                ref[h, i, base + 16 * whole * c + at : base + 16 * whole * c + at + 16, :] = value
            else:
                ref[h, i, base + 32 * whole + 8 * c : base + 32 * whole + 8 * c + 8, :] = value

        def body(i):
            for c in range(2):
                for at, rows in pieces:
                    cut = slice(at, at + rows)
                    first = masks[rows]
                    if stage == 0:
                        z = pltpu.roll(lk[1, c, i, cut, :], half, 1)
                        g = jnp.where(first, lk[2, c, i, cut, :], z)
                        store(gf, i, 0, 0, c, at, rows, g)
                        store(gb, i, 2 * dof * c, 0, 0, at, rows, g)
                    if stage == 1:
                        x = pltpu.roll(lk[3, c, i, cut, :], half, 1)
                        xr[c, i, cut, :] = x
                        store(gf, i, 2 * dof, 0, c, at, rows, jnp.where(first, cl[c, i, cut, :], x))
                    if stage == 2:
                        g = jnp.where(first, lk[0, c, i, cut, :], xr[c, i, cut, :])
                        store(gb, i, 2 * dof * c, 0, 1, at, rows, g)
                    if stage == 3:
                        z = pltpu.roll(lk[1, c, i, cut, :], half, 1)
                        store(gh, i, 0, 0, c, at, rows, jnp.where(first, lk[0, c, i, cut, :], z))

        loop(body)

    copies[5].wait()
    for c in range(2):
        v = rhs_ref[c]
        w = roll(v, half)
        rs[0, c] = jnp.where(low, v, w)
        rs[1, c] = jnp.where(low, w, v)
        xs[0, c] = zero
        xs[1, c] = zero

    for stage, needs in enumerate(((1, 2), (3, 4), (0, 6))):
        for d in needs:
            copies[d].wait()
        prepare(sa % 2, stage)

    def fold(v):
        total = v[0:8]
        for t in range(1, tiles):
            total = total + v[8 * t : 8 * t + 8]
        return total

    def gathered(slot, part):
        parts = []
        for t in range(tiles):
            total = None
            for k in range(8):
                piece = f_ref[slot, part, pl.ds(8 * 8 * t + k, 8, stride=8), :]
                total = piece if total is None else total + piece
            parts.append(total)
        return jnp.concatenate(parts, axis=0)

    def two(v):
        high = v.astype(BF16).astype(F32)
        return high, v - high

    def put_operands(slot, group, vr, vi):
        for term, (r, i) in enumerate(zip(two(vr), two(vi))):
            n = -i
            top = 16 * whole
            out = [r[16 * t : 16 * t + 16] for t in range(whole)]
            out += [i[16 * t : 16 * t + 16] for t in range(whole)]
            out += [n[16 * t : 16 * t + 16] for t in range(whole)]
            out += [jnp.concatenate([r[top:], n[top:]], axis=0), jnp.concatenate([i[top:], r[top:]], axis=0)]
            for at, value in enumerate(out):
                opf[slot, group, term, at] = value.astype(BF16)

    def forward(slot, groups, matrix):
        def operand(group, term, at):
            return opf[slot, group, term, at].astype(F32)

        real = list(range(whole)) + list(range(2 * whole, 3 * whole)) + [3 * whole]
        imag = list(range(whole, 2 * whole)) + list(range(whole)) + [3 * whole + 1]
        for o in range(dof):
            sums = [None, None]
            for group in range(groups):
                for t in range(packed):
                    m = matrix(o, group, t).astype(F32)
                    for term in range(2):
                        for part, order in enumerate((real, imag)):
                            p = m * operand(group, term, order[t])
                            sums[part] = p if sums[part] is None else sums[part] + p
            for part in range(2):
                f_ref[slot, part, 8 * o : 8 * o + 8, :] = sums[part][0:8] + sums[part][8:16]

    def backward(slot, k, matrix):
        rounds = []
        t = 0
        while t + 1 < packed:
            rounds.append([(t, 0, dof), (t + 1, 0, dof)])
            t += 2
        if t < packed:
            rounds.append([(t, 0, dof // 2), (t, dof // 2, dof)])
        done = {}
        for index, chains in enumerate(rounds):
            sums = [[None, None] for _ in chains]
            for step in range(chains[0][2] - chains[0][1]):
                if index == 0:
                    for n in range(6):
                        spread = jnp.broadcast_to(gv[k, n, pl.ds(step, 1), :], (16, lanes))
                        pk[slot, n, step] = spread.astype(BF16)
                for chain, (t, start, _) in enumerate(chains):
                    i = start + step
                    mr = matrix(i, 0, t).astype(F32)
                    mi = matrix(i, 1, t).astype(F32)
                    x = [pk[slot, n, i].astype(F32) for n in range(6)]
                    for part, terms in enumerate(
                        (
                            ((mr, x[0]), (mr, x[1]), (mi, x[2]), (mi, x[3])),
                            ((mr, x[2]), (mr, x[3]), (mi, x[4]), (mi, x[5])),
                        )
                    ):
                        for m, y in terms:
                            p = m * y
                            old = sums[chain][part]
                            sums[chain][part] = p if old is None else old + p
            for chain, (t, _, _) in enumerate(chains):
                if t in done:
                    done[t] = [a + b for a, b in zip(done[t], sums[chain])]
                else:
                    done[t] = sums[chain]
        out = []
        for group in range(2):
            out.append([])
            for part in range(2):
                parts = [done[whole * group + t][part] for t in range(whole)]
                parts.append(done[2 * whole][part][8 * group : 8 * group + 8])
                out[group].append(-signs * jnp.concatenate(parts, axis=0))
        return out

    def phase(ph, token):
        h = lax.rem(ph + sa, 2)
        other = 1 - h
        limit = steps_ref[h]
        first = (lane >= half) == ((lane * 0 + h) == 1)
        h_is_0 = (lane * 0 + h) == 0

        def ahead(v):
            n = -v
            ya = jnp.where(y_last, roll(n, (LY - 1) * LX), roll(n, -LX))
            za = jnp.where(z_last, 0.0, roll(n, -plane))
            xa = jnp.where(x_last, roll(n, LX - 1), roll(n, -1))
            return jnp.where(first, ya, za), jnp.where(first, v, xa)

        def total(v):
            return jnp.sum(jnp.sum(fold(v), axis=0, keepdims=True), axis=1, keepdims=True)

        def scale(k, q, s):
            numer_real = total(q[0] * s[0] + q[1] * s[1])
            numer_imag = total(q[0] * s[1] - q[1] * s[0])
            denom = total(q[0] * q[0] + q[1] * q[1]) + 2e-6
            live = (lane[0:1] * 0 + limit) > k
            ar = jnp.where(live, jnp.broadcast_to(numer_real / denom, (1, lanes)), 0.0)
            ai = jnp.where(live, jnp.broadcast_to(numer_imag / denom, (1, lanes)), 0.0)
            return ar, ai

        def times(a, v):
            return [a[0] * v[0] - a[1] * v[1], a[0] * v[1] + a[1] * v[0]]

        def plus(u, v):
            return [u[0] + v[0], u[1] + v[1]]

        def minus(u, v):
            return [u[0] - v[0], u[1] - v[1]]

        def keep(ref, v):
            for c in range(2):
                ref[c] = v[c]

        def kept(ref):
            return [ref[0], ref[1]]

        def apply(k, v):
            slot = lax.rem(ph + k, MR_MAX)
            gr, gi = two(signs * v[0]), two(signs * v[1])
            for term in range(2):
                gv[k, term] = gr[term]
                gv[k, 2 + term] = gi[term]
                gv[k, 4 + term] = -gr[term]
            aheads = [ahead(v[0]), ahead(v[1])]
            for group in range(2):
                put_operands(slot, group, aheads[0][group], aheads[1][group])
            back0, back2 = backward(
                slot,
                k,
                lambda i, c, t: gb[h, i, 2 * dof * c + 16 * t : 2 * dof * c + 16 * t + 16, :],
            )
            near = []
            for c in range(2):
                b, d = back0[c], back2[c]
                yb = jnp.where(y_first, roll(b, -(LY - 1) * LX), roll(b, LX))
                zb = jnp.where(z_first, 0.0, roll(b, plane))
                xb = jnp.where(x_first, roll(d, -(LX - 1)), roll(d, 1))
                u = jnp.where(first, yb, zb) + jnp.where(first, 0.0, xb)
                near.append(u + roll(u, half))
                bm_ref[k, 0, c] = jnp.where(first, roll(b, half), b)
                bm_ref[k, 1, c] = jnp.where(first, d, roll(d, half))
            forward(
                slot,
                2,
                lambda o, group, t: gf[h, o, 2 * dof * group + 16 * t : 2 * dof * group + 16 * t + 16, :],
            )
            out = []
            for c in range(2):
                u = gathered(slot, c)
                out.append(u + roll(u, half) + near[c])
            return out

        s = kept(rs.at[h])
        q = apply(0, s)
        alpha = scale(0, q, s)
        w = apply(1, q)
        e = times(alpha, s)
        s = minus(s, times(alpha, q))
        q = minus(q, times(alpha, w))
        keep(e_ref, e)
        keep(s_ref, s)
        keep(q_ref, q)
        for n in range(2):
            b = kept(bm_ref.at[0, n])
            keep(acc.at[n], times(alpha, b))
            keep(bs_ref.at[n], minus(b, times(alpha, kept(bm_ref.at[1, n]))))
        alpha = scale(1, q, s)
        w = apply(2, q)
        s, q = kept(s_ref), kept(q_ref)
        e = plus(kept(e_ref), times(alpha, s))
        s = minus(s, times(alpha, q))
        q = minus(q, times(alpha, w))
        back = []
        for n in range(2):
            b = kept(bs_ref.at[n])
            total_b = plus(kept(acc.at[n]), times(alpha, b))
            back.append((total_b, minus(b, times(alpha, kept(bm_ref.at[2, n])))))

        def pack(v):
            return jnp.where(low, v[0], v[1])

        def sender(n, where_to, src, dst):
            return pltpu.make_async_remote_copy(
                src_ref=src,
                dst_ref=dst,
                send_sem=ssem.at[ph, n],
                recv_sem=rsem.at[ph, n],
                device_id=where_to,
                device_id_type=MESH,
            )

        target = {"ta": lax.rem(ta + nt + 2 * h - 1, nt)}

        @pl.when(ph == 0)
        def _():
            pl.semaphore_wait(barrier, 4)

        alpha = scale(2, q, s)
        e_new = plus(e, times(alpha, s))
        bt = [-v for v in plus(back[1][0], times(alpha, back[1][1]))]
        sbuf[ph, 0] = jnp.where(h_is_0, pack(e_new), pack(bt))
        sends = [sender(0, target, sbuf.at[ph, 0], rbuf.at[ph, 0])]
        sends[0].start()
        bz = [-v for v in plus(back[0][0], times(alpha, back[0][1]))]
        sbuf[ph, 1] = pack(e_new)
        sbuf[ph, 2] = pack(bz)
        sends.append(sender(1, {"sa": z_prev}, sbuf.at[ph, 1], rbuf.at[ph, 1]))
        sends.append(sender(2, {"sa": z_next}, sbuf.at[ph, 2], rbuf.at[ph, 2]))
        sends[1].start()
        sends[2].start()

        left = minus(s, times(alpha, q))
        for c in range(2):
            xs[h, c] += e_new[c]
            rs[h, c] = left[c]

        @pl.when(h == 0)
        def _():
            for c in range(2):
                rs[1, c] += bt[c]

        @pl.when(h == 1)
        def _():
            for c in range(2):
                t_ref[c] = e_new[c]

        @pl.when(ph == 0)
        def _():
            for stage in range(4):
                prepare(other, stage)
            prepare(h, 3)

        def unpack(n):
            m = rbuf[ph, n]
            w = roll(m, half)
            return jnp.where(low, m, w), jnp.where(low, w, m)

        sends[1].wait()
        sends[2].wait()
        m = rbuf[ph, 2]
        near_low, near_high = roll(m, half + plane), roll(m, plane)
        rs[other, 0] += jnp.where(z_first, jnp.where(low, near_low, near_high), 0.0)
        rs[other, 1] += jnp.where(z_first, jnp.where(low, near_high, near_low), 0.0)
        m = rbuf[ph, 1]
        own, far = roll(m, half - plane), roll(m, -plane)
        zin = (
            jnp.where(z_last, jnp.where(h_is_0, own, far), 0.0),
            jnp.where(z_last, jnp.where(h_is_0, far, own), 0.0),
        )
        for c in range(2):
            z_ref[c] = zin[c]

        @pl.when(h == 0)
        def _():
            sends[0].wait()
            m = rbuf[ph, 0]
            t_ref[0] = roll(m, half)
            t_ref[1] = m

        inputs = [jnp.where(first, z_ref[c], t_ref[c]) for c in range(2)]
        slot = lax.rem(ph, MR_MAX)
        put_operands(slot, 0, inputs[0], inputs[1])
        forward(slot, 1, lambda o, group, t: gh[other, o, 16 * t : 16 * t + 16, :])
        for c in range(2):
            u = gathered(slot, c)
            rs[other, c] += u + roll(u, half)

        @pl.when(h == 1)
        def _():
            sends[0].wait()
            got_t = unpack(0)
            for c in range(2):
                rs[0, c] += got_t[c]

        return token

    lax.fori_loop(0, PHASES, phase, 0)

    for c in range(2):
        out_ref[0, c] = jnp.where(low, xs[0, c], xs[1, c])
        out_ref[1, c] = jnp.where(low, rs[0, c], rs[1, c])


def shards(nt, nz, rhs, links, clover, mr_steps):
    dof, lanes = rhs.shape[2], rhs.shape[-1]
    vmem = pl.BlockSpec(memory_space=pltpu.VMEM)
    hbm = pl.BlockSpec(memory_space=pltpu.HBM)
    operands = 3 * (dof // 16) + 2
    field = pltpu.VMEM((2, dof, lanes), F32)
    fields = pltpu.VMEM((2, 2, dof, lanes), F32)
    out = pl.pallas_call(
        functools.partial(kernel, nt, nz),
        out_shape=jax.ShapeDtypeStruct((2, 2, dof, lanes), F32),
        in_specs=[hbm, hbm, hbm, hbm],
        out_specs=vmem,
        scratch_shapes=[
            field,
            pltpu.SMEM((2,), jnp.int32),
            pltpu.VMEM((4, 2, dof, dof, lanes), BF16),
            pltpu.VMEM((2, dof, dof, lanes), BF16),
            pltpu.VMEM((2, dof, 4 * dof, lanes), BF16),
            pltpu.VMEM((2, dof, 4 * dof, lanes), BF16),
            pltpu.VMEM((2, dof, 2 * dof, lanes), BF16),
            pltpu.VMEM((2, dof, dof, lanes), BF16),
            fields,
            fields,
            field,
            field,
            field,
            fields,
            fields,
            pltpu.VMEM((MR_MAX, 2, 2, dof, lanes), F32),
            field,
            field,
            pltpu.VMEM((MR_MAX, 6, dof, lanes), F32),
            pltpu.VMEM((MR_MAX, 2, 2, operands, 16, lanes), BF16),
            pltpu.VMEM((MR_MAX, 6, dof, 16, lanes), BF16),
            pltpu.VMEM((MR_MAX, 2, 8 * dof, lanes), F32),
            pltpu.VMEM((PHASES, 3, dof, lanes), F32),
            pltpu.VMEM((PHASES, 3, dof, lanes), F32),
            pltpu.SemaphoreType.DMA((7,)),
            pltpu.SemaphoreType.DMA((PHASES, 3)),
            pltpu.SemaphoreType.DMA((PHASES, 3)),
        ],
        compiler_params=pltpu.CompilerParams(
            collective_id=0, has_side_effects=True, vmem_limit_bytes=67043328
        ),
    )(
        rhs.reshape(2, dof, lanes),
        links.reshape(4, 2, dof, dof, lanes),
        clover.reshape(2, dof, dof, lanes),
        mr_steps.reshape(2),
    )
    return out[0].reshape(rhs.shape), out[1].reshape(rhs.shape)


def solution(mesh):
    placed = (
        P(None, None, None, "ta", "sa", None),
        P(None, None, None, None, "ta", "sa", None),
        P(None, None, None, "ta", "sa", None),
        P("ta", "sa", None),
    )
    return jax.shard_map(
        functools.partial(shards, mesh.shape["ta"], mesh.shape["sa"]),
        mesh=mesh,
        in_specs=placed,
        out_specs=(P(None, None, None, "ta", "sa", None), P(None, None, None, "ta", "sa", None)),
        check_vma=False,
    )
```
